128 devices in a mesh: space: 32 (over z, y, core), freq: 4 (over x).
Axes of the slice: x: 4, y: 4, z: 4, core: 2. Of those that a mesh axis runs over, the one named last changes fastest.
Arguments:
- coeffs: bfloat16 [128, 2, 64, 49152], P('freq', None, None, 'space'), may hold values from -6 to 6
- weights: float32 [49152], P('space'), may hold values from 0.25 to 4
- mode_counts: int32 [128], replicated, may hold values from 4 to 64
- owner_order: int32 [128], replicated, may hold values from 0 to 127, as said below
Outputs:
- mode_fields: bfloat16 [128, 2, 64, 49152], P('freq', None, None, 'space')
- spectrum: float32 [128, 64], P(('space', 'freq'))
- energy: float32 [64], replicated
The draws below stay inside these ranges and needn't reach their ends.
Inputs may be any that keep to these rules, and one draw needn't show every extreme that they name: `owner_order`: A permutation of the frequencies in which slot r holds a frequency f with f // 32 == (r) % 4.
All inputs are finite; a program needn't handle non-finite values.
Results may differ from the reference program's by a relative error of at most 0.0047.
Values may be sent and summed in bfloat16 or wider, within the bound.
No kernel may reach another device: no remote copies, remote signals or barrier semaphores. Data moves between devices by JAX's collectives and lax.ppermute only.
A program may use at most 128 MiB of HBM per device.

```python
import math
import jax
import jax.numpy as jnp
from jax import lax

F = 128
B = 64
M = 64
ITERS = 3
NX = 49152
FG = 32
FPD = 1
N_FREQ = 4


def group_permutation(key_group):
    return jax.random.permutation(key_group, FG)


def fold_group(base_key, group_index):
    return jax.random.fold_in(base_key, group_index)


def draw_owner_order(key, part):
    group_keys = jax.vmap(fold_group, in_axes=(None, 0))(key, jnp.arange(N_FREQ, dtype=jnp.int32))
    permuted = jax.vmap(group_permutation)(group_keys)
    slot_ids = jnp.arange(F, dtype=jnp.int32)
    slot_group = slot_ids // FPD % N_FREQ
    slot_place = slot_ids // FPD // N_FREQ * FPD + slot_ids % FPD
    return (permuted[slot_group, slot_place] + slot_group * FG).astype(jnp.int32)


def set_ends(result, own_key, smallest, top_value):
    extent = result.shape
    place = [jax.random.randint(jax.random.fold_in(own_key, axis), (), 0, extent[axis]) for axis in range(len(extent))]
    result = result.at[tuple(place)].set(smallest)
    longest = extent.index(max(extent))
    place[longest] = (place[longest] + 1) % extent[longest]
    return result.at[tuple(place)].set(top_value)


def shard_levels(rng, dims, cuts, low, largest):
    factor_of, own = 1.0, jax.random.fold_in(rng, 6)
    for axis_at, blocks in cuts:
        steps = jnp.exp(jax.random.uniform(jax.random.fold_in(own, axis_at), (blocks,), jnp.float32, low / len(cuts), largest / len(cuts)))
        factor_of = factor_of * jnp.repeat(steps, dims[axis_at] // blocks).reshape([-1 if axis == axis_at else 1 for axis in range(len(dims))])
    return factor_of


def centred(own_key, extent, deviation, limit, cuts=(), held_as=jnp.bfloat16):
    entries = deviation * jax.random.normal(own_key, extent, jnp.float32)
    if cuts:
        entries = entries * shard_levels(own_key, extent, cuts, -0.22, 0.18)
    return jnp.clip(entries, -limit, limit).astype(held_as)


def setup_inputs(seed: int = 0) -> dict:
    arg_keys = jax.random.split(jax.random.key(seed), 5)
    coeffs = centred(arg_keys[0], (F, 2, B, NX), 1.0, 6.0, ((0, 4), (3, 32)))
    weights = jnp.clip(jnp.exp(math.log(4.0) - 2.7725887 * jax.random.uniform(arg_keys[1], (NX,), jnp.float32) ** shard_levels(arg_keys[1], (NX,), ((0, 32),), -0.2, 0.2)), 0.25, 4.0)
    mode_counts = set_ends(jax.random.randint(arg_keys[2], (F,), 4, 65), jax.random.fold_in(arg_keys[2], 1), 4, 64).astype(jnp.int32)
    owner_order = draw_owner_order(jax.random.fold_in(arg_keys[4], 71), 0)
    return dict(coeffs=coeffs, weights=weights, mode_counts=mode_counts, owner_order=owner_order)


def embed_real(products):
    half_n = products.shape[0] // 2
    real_part = products[:half_n, :half_n] + products[half_n:, half_n:]
    imag_part = products[:half_n, half_n:] - products[half_n:, :half_n]
    real_part = 0.5 * (real_part + real_part.T)
    imag_part = 0.5 * (imag_part - imag_part.T)
    upper_rows = jnp.concatenate([real_part, -imag_part], axis=1)
    bottom = jnp.concatenate([imag_part, real_part], axis=1)
    return (jnp.concatenate([upper_rows, bottom], axis=0), jnp.trace(real_part) / half_n)

def iterate(hermit, shift_val, mode_slots, sweeps):
    basis_cols = jnp.eye(hermit.shape[0], mode_slots, dtype=jnp.float32)
    for sweep_index in range(sweeps):
        image_cols = jnp.dot(hermit, basis_cols, precision=lax.Precision.HIGHEST) + shift_val * basis_cols
        gram_mat = jnp.dot(image_cols.T, image_cols, precision=lax.Precision.HIGHEST)
        lower_tri = jnp.linalg.cholesky(gram_mat)
        basis_cols = lax.linalg.triangular_solve(lower_tri, image_cols, left_side=False, lower=True, transpose_a=True)
    ritz_vals = jnp.sum(basis_cols * jnp.dot(hermit, basis_cols, precision=lax.Precision.HIGHEST), axis=0)
    return (basis_cols, ritz_vals)

def expand(basis_cols, kept_cols):
    half_n = basis_cols.shape[0] // 2
    real_cols = basis_cols[:half_n] * kept_cols
    imag_cols = basis_cols[half_n:] * kept_cols
    expander = jnp.concatenate([jnp.concatenate([real_cols, imag_cols], axis=1), jnp.concatenate([-imag_cols, real_cols], axis=1)], axis=0)
    return expander.T.astype(jnp.bfloat16)

def reference(coeffs, weights, mode_counts, owner_order):
    cell_weights = weights / NX

    def per_frequency(inputs):
        coeff_f, count_f = inputs
        weighted = (coeff_f * cell_weights).astype(jnp.bfloat16)
        flat_rows = coeff_f.reshape(2 * B, NX)
        flat_weighted = weighted.reshape(2 * B, NX)
        products = jnp.dot(flat_rows.astype(jnp.float32), flat_weighted.T.astype(jnp.float32), preferred_element_type=jnp.float32)
        hermit, shift_val = embed_real(products)
        basis_cols, ritz_vals = iterate(hermit, shift_val, M, ITERS)
        kept_cols = (jnp.arange(M, dtype=jnp.int32) < count_f).astype(jnp.float32)
        expander = expand(basis_cols, kept_cols)
        mode_field = jnp.dot(expander.astype(jnp.float32), flat_rows.astype(jnp.float32), preferred_element_type=jnp.float32).astype(jnp.bfloat16)
        return (mode_field.reshape(2, M, NX), ritz_vals * kept_cols)
    mode_fields, ritz_all = lax.map(per_frequency, (coeffs, mode_counts))
    spectrum = ritz_all[owner_order]
    energy = jnp.sum(ritz_all, axis=0) / F
    return (mode_fields, spectrum, energy)
```

```python
import functools

import jax
import jax.numpy as jnp
from jax import lax
from jax.experimental import pallas as pl
from jax.experimental.pallas import tpu as pltpu
from jax.sharding import Mesh
from jax.sharding import PartitionSpec as P

M = 64
SPACE = ("space_0", "space_1", "space_2")
PLANE = ("space_0", "space_1")
CORE = "space_2"
SPACE_FREQ = ("space_0", "space_1", "space_2", "freq")
HIGH = lax.Precision.HIGHEST
BLK = 16
PAY = 80

VMEM_SPEC = pl.BlockSpec(memory_space=pltpu.VMEM)
SMEM_SPEC = pl.BlockSpec(memory_space=pltpu.SMEM)
ANY_SPEC = pl.BlockSpec(memory_space=pl.ANY)


def nt(a, b, precision=None):
    return lax.dot_general(
        a, b, (((1,), (1,)), ((), ())), precision=precision, preferred_element_type=jnp.float32
    )


def nn(a, b, precision=None):
    return lax.dot_general(
        a, b, (((1,), (0,)), ((), ())), precision=precision, preferred_element_type=jnp.float32
    )


def iotas(shape):
    return (
        lax.broadcasted_iota(jnp.int32, shape, 0),
        lax.broadcasted_iota(jnp.int32, shape, 1),
    )


def place_of(i, half, where, order):
    core = where[1] if half == 1 else 1 - where[1]
    return order[(2 * i + core) * where[3] + where[0]] - where[0] * where[2]


def fold_pack(prod):
    sym = prod + prod.T
    top = sym[:64]
    bot = pltpu.roll(sym[64:], 64, 1)
    _, lane = iotas((64, 128))
    both = 0.5 * jnp.where(lane < 64, top + bot, top - bot)
    row, lane = iotas((32, 128))
    up, low = both[:32], both[32:]
    left = pltpu.roll(low, 96, 1)
    right = pltpu.roll(low, 32, 1)
    out = jnp.where((lane < 32) & (lane < row), left, up)
    inner = (lane >= 64) & (lane < 96)
    out = jnp.where(inner & (lane - 64 < row), left, out)
    return jnp.where(inner & (lane - 64 == row), right, out)


def unpack(packed):
    row, lane = iotas((32, 128))
    turned = jnp.concatenate([packed, jnp.zeros((96, 128), jnp.float32)], axis=0).T
    t0, t1, t2, t3 = (turned[32 * k : 32 * k + 32] for k in range(4))
    t2 = pltpu.roll(t2, 64, 1)
    t3 = pltpu.roll(t3, 64, 1)
    inner = lane - 64
    cr00 = jnp.where(lane >= row, packed, t0)
    ci00 = jnp.where(inner > row, packed, jnp.where(inner == row, 0.0, -t2))
    upper = jnp.where(lane < 32, cr00, jnp.where((lane >= 64) & (lane < 96), ci00, packed))
    diag = pltpu.roll(packed, 64, 1)
    cr11 = jnp.where(lane < row, packed, jnp.where(lane == row, diag, t0))
    ci11 = jnp.where(inner < row, packed, jnp.where(inner == row, 0.0, -t2))
    both11 = pltpu.roll(jnp.where(lane < 64, cr11, ci11), 32, 1)
    ends = jnp.where(lane < 64, t1, -t3)
    second = ((lane >= 32) & (lane < 64)) | (lane >= 96)
    lower = jnp.where(second, both11, ends)
    return jnp.concatenate([upper, lower], axis=0)


def gram_kernel(where, order, cells_ref, coeffs, send_ref, own_ref, kept_ref, prods, sems):
    count = send_ref.shape[0]

    def copy(i, half):
        k = i + half * count
        src = coeffs.at[place_of(i, half, where, order)]
        return pltpu.make_async_copy(src, kept_ref.at[k], sems.at[k])

    for half in (0, 1):

        @pl.loop(0, count)
        def _(i, half=half):
            copy(i, half).start()

    cells = cells_ref[...].reshape(1, -1) / where[5].astype(jnp.float32)
    for half, out_ref in ((0, send_ref), (1, own_ref)):

        @pl.loop(0, count)
        def _(i, half=half):
            copy(i, half).wait()
            k = i + half * count
            rows = kept_ref[k]
            weighted = (rows.astype(jnp.float32) * cells).astype(jnp.bfloat16)
            prods[i] = nt(rows, weighted)

        @pl.loop(0, count, step=4)
        def _(i, out_ref=out_ref):
            for j in range(4):
                out_ref[i + j] = fold_pack(prods[i + j])


def orth_rows(zt, floor=0.0):
    n = zt.shape[0]
    gram = nt(zt, zt, HIGH)
    rest_g, rest_z = gram, zt
    row, _ = iotas((BLK, 128))
    outs = []
    for blk in range(n // BLK):
        r0 = BLK * blk
        head_g, head_z = rest_g[:BLK], rest_z[:BLK]
        tail_g, tail_z = rest_g[BLK:], rest_z[BLK:]
        more = tail_g.shape[0]
        cols = [
            jnp.broadcast_to(head_g[:, r0 + j : r0 + j + 1], (BLK, 128)) for j in range(BLK)
        ]
        tails = [
            jnp.broadcast_to(tail_g[:, r0 + j : r0 + j + 1], (more, 128)) if more else None
            for j in range(BLK)
        ]
        acc = jnp.zeros((BLK, 128), jnp.float32)
        for j in range(BLK):
            here = row == j
            pivot = jnp.broadcast_to(cols[j][j : j + 1], (BLK, 128))
            if floor:
                pivot = jnp.maximum(pivot, floor)
            acc = jnp.where(here, head_z * lax.rsqrt(pivot), acc)
            inv = 1.0 / pivot

            def eliminated(x, j=j, here=here, inv=inv, width=128):
                lead = jnp.broadcast_to(x[j : j + 1], x.shape) * inv[:, :width]
                return jnp.where(here[:, :width], lead, x - cols[j][:, :width] * lead)

            head_z = eliminated(head_z)
            if more:
                head_g = eliminated(head_g, width=n)
            for jj in range(j + 1, BLK):
                cols[jj] = eliminated(cols[jj])
        outs.append(acc)
        for j in range(BLK if more else 0):
            tail_z = tail_z - tails[j] * head_z[j : j + 1]
            tail_g = tail_g - tails[j][:, :n] * head_g[j : j + 1]
        rest_g, rest_z = tail_g, tail_z
    return jnp.concatenate(outs, axis=0)


def solve_kernel(where, order, counts, parts_ref, pay_ref, ritz_ref):
    summed = parts_ref[0]
    for i in range(1, parts_ref.shape[0]):
        summed = summed + parts_ref[i]
    both = unpack(summed)
    row, lane = iotas((64, 128))
    shift = jnp.sum(jnp.where(row == lane, both, 0.0), keepdims=True) * (1.0 / 64.0)
    hermit = jnp.concatenate([jnp.where(lane < 64, both, -both), pltpu.roll(both, 64, 1)], axis=0)
    row, lane = iotas((128, 128))
    shifted = hermit * (1.0 / shift) + jnp.where(row == lane, 1.0, 0.0)
    basis = orth_rows(nn(shifted[:64], shifted, HIGH), 0.25)
    basis = orth_rows(nn(basis, shifted, HIGH))
    quad = basis * nn(basis, hermit, HIGH)
    ritz = nt(jnp.ones((8, 128), jnp.float32), quad, HIGH)
    slot = where[4]
    kept = counts[order[slot]]
    _, lane = iotas((8, 64))
    ritz = jnp.where(lane < kept, ritz, 0.0)
    ritz_ref[...] = ritz[:1]
    row, _ = iotas((64, 128))
    sent = jnp.where(row < kept, basis, 0.0).astype(jnp.bfloat16)
    one = ritz.astype(jnp.bfloat16)
    left = ritz - one.astype(jnp.float32)
    two = left.astype(jnp.bfloat16)
    three = left - two.astype(jnp.float32)
    row, _ = iotas((8, 128))
    upper = jnp.concatenate([one.astype(jnp.float32), two.astype(jnp.float32)], axis=1)
    lower = jnp.concatenate([three, jnp.zeros_like(three)], axis=1)
    tail = jnp.where(row == 0, upper, jnp.where(row == 1, lower, 0.0))
    tail = jnp.concatenate([tail, jnp.zeros((8, 128), jnp.float32)], axis=0).astype(jnp.bfloat16)
    for i in range(pay_ref.shape[0]):
        pay_ref[i, :64] = sent
        pay_ref[i, 64:] = tail


def modes_kernel(half, where, order, bases_ref, kept_ref, *rest):
    out, expanders, stage, sems = rest[-4:]
    count = bases_ref.shape[0]
    slots = stage.shape[0]
    _, lane = iotas((64, 128))
    for i in range(count):
        basis = bases_ref[i, :64].astype(jnp.float32)
        expanders[i, :64] = jnp.where(lane < 64, basis, -basis).astype(jnp.bfloat16)
        expanders[i, 64:] = pltpu.roll(basis, 64, 1).astype(jnp.bfloat16)

    def copy(i):
        s = lax.rem(i, slots)
        return pltpu.make_async_copy(stage.at[s], out.at[place_of(i, half, where, order)], sems.at[s])

    @pl.loop(0, count)
    def _(i):
        @pl.when(i >= slots)
        def _():
            copy(i - slots).wait()

        stage[lax.rem(i, slots)] = nn(expanders[i], kept_ref[i + half * count]).astype(jnp.bfloat16)
        copy(i).start()

    for i in range(count - slots, count):
        copy(i).wait()


def compiler(mib):
    return pltpu.CompilerParams(vmem_limit_bytes=mib * 2**20)


def shards(coeffs, weights, mode_counts, owner_order):
    fgroup, _, blocks, points = coeffs.shape
    freqs = lax.axis_size("freq")
    group, core = lax.axis_index("freq"), lax.axis_index(CORE)
    space = lax.axis_index(SPACE)
    plane = lax.axis_size(PLANE)
    as32 = functools.partial(jnp.asarray, dtype=jnp.int32)
    where = jnp.stack(
        [as32(group), as32(core), as32(fgroup), as32(freqs), as32(space * freqs + group), as32(points * lax.axis_size(SPACE))]
    )
    rows = coeffs.reshape(fgroup, 2 * blocks, points)
    f32, bf16 = jnp.float32, jnp.bfloat16
    packed = jax.ShapeDtypeStruct((plane, 32, 128), f32)
    send, own, kept = pl.pallas_call(
        gram_kernel,
        out_shape=(packed, packed, pltpu.VMEM((fgroup, 2 * blocks, points), bf16)),
        in_specs=[SMEM_SPEC, SMEM_SPEC, VMEM_SPEC, ANY_SPEC],
        out_specs=(VMEM_SPEC, VMEM_SPEC, VMEM_SPEC),
        scratch_shapes=[
            pltpu.VMEM((plane, 128, 128), f32),
            pltpu.SemaphoreType.DMA((fgroup,)),
        ],
        compiler_params=compiler(32),
        name="gram",
    )(where, owner_order, weights, rows)
    swap = [(0, 1), (1, 0)]
    mine = own + lax.ppermute(send, CORE, swap)
    parts = lax.all_to_all(mine, PLANE, 0, 0, tiled=True)
    payload, ritz = pl.pallas_call(
        solve_kernel,
        out_shape=(
            jax.ShapeDtypeStruct((plane, PAY, 128), bf16),
            jax.ShapeDtypeStruct((1, M), f32),
        ),
        in_specs=[SMEM_SPEC, SMEM_SPEC, SMEM_SPEC, VMEM_SPEC],
        out_specs=(VMEM_SPEC, VMEM_SPEC),
        compiler_params=compiler(16),
        name="solve",
    )(where, owner_order, mode_counts, parts)
    bases = lax.all_to_all(payload, PLANE, 0, 0, tiled=True)
    others = lax.ppermute(bases, CORE, swap)

    def total(b):
        tail = b[:, 64:66].astype(f32).sum(axis=0)
        return tail[0, :64] + tail[0, 64:] + tail[1, :64]

    def modes(half, bases, *into):
        return pl.pallas_call(
            functools.partial(modes_kernel, half),
            out_shape=jax.ShapeDtypeStruct((fgroup, 2 * blocks, points), bf16),
            in_specs=[SMEM_SPEC, SMEM_SPEC, VMEM_SPEC, VMEM_SPEC] + [ANY_SPEC] * len(into),
            out_specs=ANY_SPEC,
            scratch_shapes=[
                pltpu.VMEM((plane, 128, 128), bf16),
                pltpu.VMEM((4, 2 * blocks, points), bf16),
                pltpu.SemaphoreType.DMA((4,)),
            ],
            input_output_aliases={4: 0} if into else {},
            compiler_params=compiler(16),
            name="modes%d" % half,
        )(where, owner_order, bases, kept, *into)

    fields = modes(1, bases)
    fields = modes(0, others, fields)
    energy = total(bases) + total(others)
    ring = [
        lax.ppermute(energy, "freq", [(i, (i + k) % freqs) for i in range(freqs)])
        for k in range(1, freqs)
    ]
    energy = functools.reduce(jnp.add, ring, energy) / (fgroup * freqs)
    return (fields.reshape(fgroup, 2, M, points), ritz, energy)


def solution(mesh):
    split = Mesh(
        mesh.devices.reshape(4, 4, 2, mesh.shape["freq"]), ("space_0", "space_1", "space_2", "freq")
    )
    placed = (P("freq", None, None, SPACE), P(SPACE), P(), P())
    return jax.shard_map(
        shards,
        mesh=split,
        in_specs=placed,
        out_specs=(P("freq", None, None, SPACE), P(SPACE_FREQ, None), P()),
        check_vma=False,
    )
```

```python
import functools

import jax
import jax.numpy as jnp
from jax import lax
from jax.experimental import pallas as pl
from jax.experimental.pallas import tpu as pltpu
from jax.sharding import Mesh
from jax.sharding import PartitionSpec as P

M = 64
ITERS = 3
SPACE = ("space_0", "space_1", "space_2")
PLANE = ("space_0", "space_1")
CORE = "space_2"
SPACE_FREQ = ("space_0", "space_1", "space_2", "freq")
HIGH = lax.Precision.HIGHEST
BLK = 16
PAY = 80
UNROLL = 4
FLIGHT = 4

VMEM_SPEC = pl.BlockSpec(memory_space=pltpu.VMEM)
ANY_SPEC = pl.BlockSpec(memory_space=pl.ANY)
SMEM_SPEC = pl.BlockSpec(memory_space=pltpu.SMEM)
HBM_SPEC = pl.BlockSpec(memory_space=pltpu.HBM)


def nt(a, b, precision=None):
    return lax.dot_general(
        a, b, (((1,), (1,)), ((), ())), precision=precision, preferred_element_type=jnp.float32
    )


def nn(a, b, precision=None):
    return lax.dot_general(
        a, b, (((1,), (0,)), ((), ())), precision=precision, preferred_element_type=jnp.float32
    )


def iotas(shape):
    return (
        lax.broadcasted_iota(jnp.int32, shape, 0),
        lax.broadcasted_iota(jnp.int32, shape, 1),
    )


def here():
    group, core = lax.axis_index("freq"), lax.axis_index(CORE)
    plane = lax.axis_index(PLANE[0]) * lax.axis_size(PLANE[1]) + lax.axis_index(PLANE[1])
    return group, core, plane


def slot_of(plane, core, group):
    return (plane * lax.axis_size(CORE) + core) * lax.axis_size("freq") + group


def place_of(i, half, order, per_group):
    group, core, _ = here()
    return order[slot_of(i, core if half == 1 else 1 - core, group)] - group * per_group


def fold_pack(prod):
    sym = prod + prod.T
    top = sym[:64]
    bot = pltpu.roll(sym[64:], 64, 1)
    _, lane = iotas((64, 128))
    both = 0.5 * jnp.where(lane < 64, top + bot, top - bot)
    row, lane = iotas((32, 128))
    up, low = both[:32], both[32:]
    left = pltpu.roll(low, 96, 1)
    right = pltpu.roll(low, 32, 1)
    out = jnp.where((lane < 32) & (lane < row), left, up)
    inner = (lane >= 64) & (lane < 96)
    out = jnp.where(inner & (lane - 64 < row), left, out)
    return jnp.where(inner & (lane - 64 == row), right, out)


def unpack(packed):
    row, lane = iotas((32, 128))
    turned = jnp.concatenate([packed, jnp.zeros((96, 128), jnp.float32)], axis=0).T
    t0, t1, t2, t3 = (turned[32 * k : 32 * k + 32] for k in range(4))
    t2 = pltpu.roll(t2, 64, 1)
    t3 = pltpu.roll(t3, 64, 1)
    inner = lane - 64
    cr00 = jnp.where(lane >= row, packed, t0)
    ci00 = jnp.where(inner > row, packed, jnp.where(inner == row, 0.0, -t2))
    upper = jnp.where(lane < 32, cr00, jnp.where((lane >= 64) & (lane < 96), ci00, packed))
    diag = pltpu.roll(packed, 64, 1)
    cr11 = jnp.where(lane < row, packed, jnp.where(lane == row, diag, t0))
    ci11 = jnp.where(inner < row, packed, jnp.where(inner == row, 0.0, -t2))
    both11 = pltpu.roll(jnp.where(lane < 64, cr11, ci11), 32, 1)
    ends = jnp.where(lane < 64, t1, -t3)
    second = ((lane >= 32) & (lane < 64)) | (lane >= 96)
    lower = jnp.where(second, both11, ends)
    return jnp.concatenate([upper, lower], axis=0)


def gram_kernel(order_hbm, counts_hbm, cells_hbm, coeffs, *rest):
    send_ref, own_ref, kept_ref, order, counts, cells, wide, packs, even, odd, side, sems = rest
    count = kept_ref.shape[0]
    chunks = count // UNROLL

    def fetch(k):
        part = pl.ds(k * UNROLL, UNROLL)
        return pltpu.make_async_copy(coeffs.at[part], kept_ref.at[part], sems.at[k])

    take_order = pltpu.make_async_copy(order_hbm, order, side.at[0])
    take_cells = pltpu.make_async_copy(cells_hbm, cells, side.at[1])
    take_counts = pltpu.make_async_copy(counts_hbm, counts, side.at[2])
    take_cells.start()
    for k in range(FLIGHT):
        fetch(k).start()
    take_order.start()
    take_counts.start()
    take_cells.wait()
    total = cells.shape[-1] * lax.axis_size(SPACE)
    wide[...] = jnp.broadcast_to(cells[...].reshape(1, -1) / total, wide.shape)

    def product(f):
        rows = kept_ref[f]
        scaled = rows.astype(jnp.float32).reshape(-1, *wide.shape) * wide[...]
        return nt(rows, scaled.reshape(rows.shape).astype(jnp.bfloat16))

    def arrived(k):
        fetch(k).wait()

        @pl.when(k + FLIGHT < chunks)
        def _():
            fetch(k + FLIGHT).start()

    def chunk(k, done, fill):
        for j in range(UNROLL):
            packs[(k - 1) * UNROLL + j] = fold_pack(done[j])
            fill[j] = product(k * UNROLL + j)

    arrived(0)
    for j in range(UNROLL):
        even[j] = product(j)

    @pl.loop(1, chunks - 1, step=2)
    def _(k):
        arrived(k)
        arrived(k + 1)
        chunk(k, even, odd)
        chunk(k + 1, odd, even)

    arrived(chunks - 1)
    chunk(chunks - 1, even, odd)
    for j in range(UNROLL):
        packs[count - UNROLL + j] = fold_pack(odd[j])
    take_order.wait()
    take_counts.wait()
    for half, out_ref in ((0, send_ref), (1, own_ref)):
        for i in range(count // 2):
            out_ref[i] = packs[place_of(i, half, order, count)]


def orth_rows(zt):
    n = zt.shape[0]
    gram = nt(zt, zt, HIGH)
    rest_g, rest_z = gram, zt
    row, _ = iotas((BLK, 128))
    outs = []
    for blk in range(n // BLK):
        r0 = BLK * blk
        head_g, head_z = rest_g[:BLK], rest_z[:BLK]
        more = n - r0 - BLK
        tail_g, tail_z = (rest_g[BLK:], rest_z[BLK:]) if more else (None, None)
        cols = [
            jnp.broadcast_to(head_g[:, r0 + j : r0 + j + 1], (BLK, 128)) for j in range(BLK)
        ]
        tails = [
            jnp.broadcast_to(tail_g[:, r0 + j : r0 + j + 1], (more, 128)) if more else None
            for j in range(BLK)
        ]
        acc = jnp.zeros((BLK, 128), jnp.float32)
        for j in range(BLK):
            here = row == j
            pivot = jnp.broadcast_to(cols[j][j : j + 1], (BLK, 128))
            acc = jnp.where(here, head_z * lax.rsqrt(pivot), acc)
            inv = 1.0 / pivot

            def eliminated(x, j=j, here=here, inv=inv, width=128):
                lead = jnp.broadcast_to(x[j : j + 1], x.shape) * inv[:, :width]
                return jnp.where(here[:, :width], lead, x - cols[j][:, :width] * lead)

            head_z = eliminated(head_z)
            if more:
                head_g = eliminated(head_g, width=n)
            for jj in range(j + 1, BLK):
                cols[jj] = eliminated(cols[jj])
        outs.append(acc)
        for j in range(BLK if more else 0):
            tail_z = tail_z - tails[j] * head_z[j : j + 1]
            tail_g = tail_g - tails[j][:, :n] * head_g[j : j + 1]
        rest_g, rest_z = tail_g, tail_z
    return jnp.concatenate(outs, axis=0)


def solve_kernel(order, counts, parts_ref, pay_ref, ritz_ref):
    summed = parts_ref[0]
    for i in range(1, parts_ref.shape[0]):
        summed = summed + parts_ref[i]
    both = unpack(summed)
    row, lane = iotas((64, 128))
    trace = jnp.sum(jnp.where(row == lane, both, 0.0)) * (1.0 / 64.0)
    shift = jnp.full((1, 1), trace)
    hermit = jnp.concatenate([jnp.where(lane < 64, both, -both), pltpu.roll(both, 64, 1)], axis=0)
    row, lane = iotas((128, 128))
    eye = jnp.where(row == lane, 1.0, 0.0)
    shifted = hermit * (1.0 / shift) + eye
    spread = jnp.sum(both * both) * 2.0
    mild = spread <= 512.0 * trace * trace
    start = jnp.where(mild, shifted[:64], eye[:64])
    sweeps = jnp.where(mild, ITERS - 1, ITERS)
    basis = lax.fori_loop(
        0, sweeps, lambda _, rows: orth_rows(nn(rows, shifted, HIGH)), start
    )
    quad = basis * nn(basis, hermit, HIGH)
    ritz = nt(jnp.ones((8, 128), jnp.float32), quad, HIGH)
    group, core, plane = here()
    kept = counts[order[slot_of(plane, core, group)]]
    _, lane = iotas((8, 64))
    ritz = jnp.where(lane < kept, ritz, 0.0)
    ritz_ref[...] = ritz[:1]
    row, _ = iotas((64, 128))
    sent = jnp.where(row < kept, basis, 0.0).astype(jnp.bfloat16)
    one = ritz.astype(jnp.bfloat16)
    left = ritz - one.astype(jnp.float32)
    two = left.astype(jnp.bfloat16)
    three = left - two.astype(jnp.float32)
    row, _ = iotas((8, 128))
    upper = jnp.concatenate([one.astype(jnp.float32), two.astype(jnp.float32)], axis=1)
    lower = jnp.concatenate([three, jnp.zeros_like(three)], axis=1)
    tail = jnp.where(row == 0, upper, jnp.where(row == 1, lower, 0.0))
    tail = jnp.concatenate([tail, jnp.zeros((8, 128), jnp.float32)], axis=0).astype(jnp.bfloat16)
    for i in range(pay_ref.shape[0]):
        pay_ref[i, :64] = sent
        pay_ref[i, 64:] = tail


def modes_kernel(order, own_ref, other_ref, kept_ref, out, expanders, stage, sems):
    count = kept_ref.shape[0]
    _, lane = iotas((64, 128))
    for half, bases_ref in ((1, own_ref), (0, other_ref)):
        for i in range(count // 2):
            k = i + (1 - half) * (count // 2)
            basis = bases_ref[i, :64].astype(jnp.float32)
            expanders[k, :64] = jnp.where(lane < 64, basis, -basis).astype(jnp.bfloat16)
            expanders[k, 64:] = pltpu.roll(basis, 64, 1).astype(jnp.bfloat16)
    group, core, _ = here()

    def place(k):
        far = lax.div(k, count // 2)
        i = k - far * (count // 2)
        return order[slot_of(i, core + far * (1 - 2 * core), group)] - group * count

    def copy(i):
        return pltpu.make_async_copy(stage.at[i], out.at[place(i)], sems.at[i])

    @pl.loop(0, count, step=UNROLL)
    def _(i):
        for j in range(UNROLL):
            rows = kept_ref[place(i + j)]
            stage[i + j] = nn(expanders[i + j], rows).astype(jnp.bfloat16)
            copy(i + j).start()

    @pl.loop(0, count)
    def _(i):
        copy(i).wait()


def compiler(mib):
    return pltpu.CompilerParams(vmem_limit_bytes=mib * 2**20)


def shards(coeffs, weights, mode_counts, owner_order):
    fgroup, _, blocks, points = coeffs.shape
    freqs = lax.axis_size("freq")
    plane = lax.axis_size(PLANE)
    slots = fgroup * freqs
    rows = coeffs.reshape(fgroup, 2 * blocks, points)
    f32, bf16 = jnp.float32, jnp.bfloat16
    packed = jax.ShapeDtypeStruct((plane, 32, 128), f32)
    in_hbm = [
        pltpu.with_memory_space_constraint(x, pltpu.HBM)
        for x in (owner_order, mode_counts, weights)
    ]
    send, own, kept, order, counts = pl.pallas_call(
        gram_kernel,
        out_shape=(
            packed,
            packed,
            pltpu.VMEM((fgroup, 2 * blocks, points), bf16),
            pltpu.SMEM((slots,), jnp.int32),
            pltpu.SMEM((slots,), jnp.int32),
        ),
        in_specs=[HBM_SPEC] * 4,
        out_specs=(VMEM_SPEC, VMEM_SPEC, VMEM_SPEC, SMEM_SPEC, SMEM_SPEC),
        scratch_shapes=[
            pltpu.VMEM((points,), f32),
            pltpu.VMEM((8, points), f32),
            pltpu.VMEM((fgroup, 32, 128), f32),
            pltpu.VMEM((UNROLL, 128, 128), f32),
            pltpu.VMEM((UNROLL, 128, 128), f32),
            pltpu.SemaphoreType.DMA((3,)),
            pltpu.SemaphoreType.DMA((fgroup // UNROLL,)),
        ],
        compiler_params=compiler(32),
        name="gram",
    )(*in_hbm, rows)
    swap = [(0, 1), (1, 0)]
    mine = own + lax.ppermute(send, CORE, swap)
    parts = lax.all_to_all(mine, PLANE, 0, 0, tiled=True)
    payload, ritz = pl.pallas_call(
        solve_kernel,
        out_shape=(pltpu.VMEM((plane, PAY, 128), bf16), pltpu.VMEM((1, M), f32)),
        in_specs=[SMEM_SPEC, SMEM_SPEC, VMEM_SPEC],
        out_specs=(VMEM_SPEC, VMEM_SPEC),
        compiler_params=compiler(16),
        name="solve",
    )(order, counts, parts)
    bases = lax.all_to_all(payload, PLANE, 0, 0, tiled=True)
    others = lax.ppermute(bases, CORE, swap)

    def total(b):
        tail = b[:, 64:66].astype(f32).sum(axis=0)
        return tail[0, :64] + tail[0, 64:] + tail[1, :64]

    fields = pl.pallas_call(
        modes_kernel,
        out_shape=jax.ShapeDtypeStruct((fgroup, 2 * blocks, points), bf16),
        in_specs=[SMEM_SPEC, VMEM_SPEC, VMEM_SPEC, VMEM_SPEC],
        out_specs=HBM_SPEC,
        scratch_shapes=[
            pltpu.VMEM((fgroup, 128, 128), bf16),
            pltpu.VMEM((fgroup, 2 * blocks, points), bf16),
            pltpu.SemaphoreType.DMA((fgroup,)),
        ],
        compiler_params=compiler(16),
        name="modes",
    )(order, bases, others, kept)
    energy = total(bases) + total(others)
    ring = [
        lax.ppermute(energy, "freq", [(i, (i + k) % freqs) for i in range(freqs)])
        for k in range(1, freqs)
    ]
    energy = functools.reduce(jnp.add, ring, energy) / (fgroup * freqs)
    return (fields.reshape(fgroup, 2, M, points), ritz, energy)


def solution(mesh):
    split = Mesh(
        mesh.devices.reshape(4, 4, 2, mesh.shape["freq"]), ("space_0", "space_1", "space_2", "freq")
    )
    placed = (P("freq", None, None, SPACE), P(SPACE), P(), P())
    return jax.shard_map(
        shards,
        mesh=split,
        in_specs=placed,
        out_specs=(P("freq", None, None, SPACE), P(SPACE_FREQ, None), P()),
        check_vma=False,
    )
```

```python
import functools

import jax
import jax.numpy as jnp
from jax import lax
from jax.experimental import pallas as pl
from jax.experimental.pallas import tpu as pltpu
from jax.sharding import Mesh
from jax.sharding import PartitionSpec as P

M = 64
ITERS = 3
SPACE = ("space_0", "space_1", "space_2")
PLANE = ("space_0", "space_1")
CORE = "space_2"
SPACE_FREQ = ("space_0", "space_1", "space_2", "freq")
HIGH = lax.Precision.HIGHEST
BLK = 16
PAY = 80
UNROLL = 4
FLIGHT = 4

VMEM_SPEC = pl.BlockSpec(memory_space=pltpu.VMEM)
ANY_SPEC = pl.BlockSpec(memory_space=pl.ANY)
SMEM_SPEC = pl.BlockSpec(memory_space=pltpu.SMEM)
HBM_SPEC = pl.BlockSpec(memory_space=pltpu.HBM)


def nt(a, b, precision=None):
    return lax.dot_general(
        a, b, (((1,), (1,)), ((), ())), precision=precision, preferred_element_type=jnp.float32
    )


def nn(a, b, precision=None):
    return lax.dot_general(
        a, b, (((1,), (0,)), ((), ())), precision=precision, preferred_element_type=jnp.float32
    )


def iotas(shape):
    return (
        lax.broadcasted_iota(jnp.int32, shape, 0),
        lax.broadcasted_iota(jnp.int32, shape, 1),
    )


def here():
    group, core = lax.axis_index("freq"), lax.axis_index(CORE)
    plane = lax.axis_index(PLANE[0]) * lax.axis_size(PLANE[1]) + lax.axis_index(PLANE[1])
    return group, core, plane


def slot_of(plane, core, group):
    return (plane * lax.axis_size(CORE) + core) * lax.axis_size("freq") + group


def place_of(i, half, order, per_group):
    group, core, _ = here()
    return order[slot_of(i, core if half == 1 else 1 - core, group)] - group * per_group


def fold_pack(prod):
    sym = prod + prod.T
    top = sym[:64]
    bot = pltpu.roll(sym[64:], 64, 1)
    _, lane = iotas((64, 128))
    both = 0.5 * jnp.where(lane < 64, top + bot, top - bot)
    row, lane = iotas((32, 128))
    up, low = both[:32], both[32:]
    left = pltpu.roll(low, 96, 1)
    right = pltpu.roll(low, 32, 1)
    out = jnp.where((lane < 32) & (lane < row), left, up)
    inner = (lane >= 64) & (lane < 96)
    out = jnp.where(inner & (lane - 64 < row), left, out)
    return jnp.where(inner & (lane - 64 == row), right, out)


def unpack(packed):
    row, lane = iotas((32, 128))
    turned = jnp.concatenate([packed, jnp.zeros((96, 128), jnp.float32)], axis=0).T
    t0, t1, t2, t3 = (turned[32 * k : 32 * k + 32] for k in range(4))
    t2 = pltpu.roll(t2, 64, 1)
    t3 = pltpu.roll(t3, 64, 1)
    inner = lane - 64
    cr00 = jnp.where(lane >= row, packed, t0)
    ci00 = jnp.where(inner > row, packed, jnp.where(inner == row, 0.0, -t2))
    upper = jnp.where(lane < 32, cr00, jnp.where((lane >= 64) & (lane < 96), ci00, packed))
    diag = pltpu.roll(packed, 64, 1)
    cr11 = jnp.where(lane < row, packed, jnp.where(lane == row, diag, t0))
    ci11 = jnp.where(inner < row, packed, jnp.where(inner == row, 0.0, -t2))
    both11 = pltpu.roll(jnp.where(lane < 64, cr11, ci11), 32, 1)
    ends = jnp.where(lane < 64, t1, -t3)
    second = ((lane >= 32) & (lane < 64)) | (lane >= 96)
    lower = jnp.where(second, both11, ends)
    return jnp.concatenate([upper, lower], axis=0)


def gram_kernel(order_hbm, counts_hbm, cells_hbm, coeffs, *rest):
    send_ref, own_ref, kept_ref, order, counts, cells, wide, packs, even, odd, side, sems = rest
    count = kept_ref.shape[0]
    chunks = count // UNROLL

    def fetch(k):
        part = pl.ds(k * UNROLL, UNROLL)
        return pltpu.make_async_copy(coeffs.at[part], kept_ref.at[part], sems.at[k])

    take_order = pltpu.make_async_copy(order_hbm, order, side.at[0])
    take_cells = pltpu.make_async_copy(cells_hbm, cells, side.at[1])
    take_counts = pltpu.make_async_copy(counts_hbm, counts, side.at[2])
    take_cells.start()
    for k in range(FLIGHT):
        fetch(k).start()
    take_order.start()
    take_counts.start()
    take_cells.wait()
    total = cells.shape[-1] * lax.axis_size(SPACE)
    wide[...] = jnp.broadcast_to(cells[...].reshape(1, -1) / total, wide.shape)

    def product(f):
        rows = kept_ref[f]
        scaled = rows.astype(jnp.float32).reshape(-1, *wide.shape) * wide[...]
        return nt(rows, scaled.reshape(rows.shape).astype(jnp.bfloat16))

    def arrived(k):
        fetch(k).wait()

        @pl.when(k + FLIGHT < chunks)
        def _():
            fetch(k + FLIGHT).start()

    def chunk(k, done, fill):
        for j in range(UNROLL):
            packs[(k - 1) * UNROLL + j] = fold_pack(done[j])
            fill[j] = product(k * UNROLL + j)

    arrived(0)
    for j in range(UNROLL):
        even[j] = product(j)

    @pl.loop(1, chunks - 1, step=2)
    def _(k):
        arrived(k)
        arrived(k + 1)
        chunk(k, even, odd)
        chunk(k + 1, odd, even)

    arrived(chunks - 1)
    chunk(chunks - 1, even, odd)
    for j in range(UNROLL):
        packs[count - UNROLL + j] = fold_pack(odd[j])
    take_order.wait()
    take_counts.wait()
    for half, out_ref in ((0, send_ref), (1, own_ref)):
        for i in range(count // 2):
            out_ref[i] = packs[place_of(i, half, order, count)]


def orth_rows(zt, held):
    n = zt.shape[0]
    gram = nt(zt, zt, HIGH)
    rest_g, rest_z = gram, zt
    row, _ = iotas((BLK, 128))
    outs = []
    for blk in range(n // BLK):
        r0 = BLK * blk
        head_g, head_z = rest_g[:BLK], rest_z[:BLK]
        more = n - r0 - BLK
        tail_g, tail_z = (rest_g[BLK:], rest_z[BLK:]) if more else (None, None)
        for j in range(BLK):
            held[j] = jnp.broadcast_to(head_g[:, r0 + j : r0 + j + 1], (BLK, 128))
        cols = [held[j] for j in range(BLK)]
        tails = [
            jnp.broadcast_to(tail_g[:, r0 + j : r0 + j + 1], (more, 128)) if more else None
            for j in range(BLK)
        ]
        acc = jnp.zeros((BLK, 128), jnp.float32)
        for j in range(BLK):
            here = row == j
            pivot = jnp.broadcast_to(cols[j][j : j + 1], (BLK, 128))
            acc = jnp.where(here, head_z * lax.rsqrt(pivot), acc)
            inv = 1.0 / pivot

            def eliminated(x, j=j, here=here, inv=inv, width=128):
                lead = jnp.broadcast_to(x[j : j + 1], x.shape) * inv[:, :width]
                return jnp.where(here[:, :width], lead, x - cols[j][:, :width] * lead)

            head_z = eliminated(head_z)
            if more:
                head_g = eliminated(head_g, width=n)
            for jj in range(j + 1, BLK):
                cols[jj] = eliminated(cols[jj])
        outs.append(acc)
        for j in range(BLK if more else 0):
            tail_z = tail_z - tails[j] * head_z[j : j + 1]
            tail_g = tail_g - tails[j][:, :n] * head_g[j : j + 1]
        rest_g, rest_z = tail_g, tail_z
    return jnp.concatenate(outs, axis=0)


def solve_kernel(order, counts, parts_ref, pay_ref, ritz_ref, held):
    summed = parts_ref[0]
    for i in range(1, parts_ref.shape[0]):
        summed = summed + parts_ref[i]
    both = unpack(summed)
    row, lane = iotas((64, 128))
    trace = jnp.sum(jnp.where(row == lane, both, 0.0)) * (1.0 / 64.0)
    shift = jnp.full((1, 1), trace)
    hermit = jnp.concatenate([jnp.where(lane < 64, both, -both), pltpu.roll(both, 64, 1)], axis=0)
    row, lane = iotas((128, 128))
    eye = jnp.where(row == lane, 1.0, 0.0)
    shifted = hermit * (1.0 / shift) + eye
    spread = jnp.sum(both * both) * 2.0
    mild = spread <= 512.0 * trace * trace
    start = jnp.where(mild, shifted[:64], eye[:64])
    sweeps = jnp.where(mild, ITERS - 1, ITERS)
    basis = lax.fori_loop(
        0, sweeps, lambda _, rows: orth_rows(nn(rows, shifted, HIGH), held), start
    )
    quad = basis * nn(basis, hermit, HIGH)
    ritz = nt(jnp.ones((8, 128), jnp.float32), quad, HIGH)
    group, core, plane = here()
    kept = counts[order[slot_of(plane, core, group)]]
    _, lane = iotas((8, 64))
    ritz = jnp.where(lane < kept, ritz, 0.0)
    ritz_ref[...] = ritz[:1]
    row, _ = iotas((64, 128))
    sent = jnp.where(row < kept, basis, 0.0).astype(jnp.bfloat16)
    one = ritz.astype(jnp.bfloat16)
    left = ritz - one.astype(jnp.float32)
    two = left.astype(jnp.bfloat16)
    three = left - two.astype(jnp.float32)
    row, _ = iotas((8, 128))
    upper = jnp.concatenate([one.astype(jnp.float32), two.astype(jnp.float32)], axis=1)
    lower = jnp.concatenate([three, jnp.zeros_like(three)], axis=1)
    tail = jnp.where(row == 0, upper, jnp.where(row == 1, lower, 0.0))
    tail = jnp.concatenate([tail, jnp.zeros((8, 128), jnp.float32)], axis=0).astype(jnp.bfloat16)
    for i in range(pay_ref.shape[0]):
        pay_ref[i, :64] = sent
        pay_ref[i, 64:] = tail


def modes_kernel(half, order, bases_ref, kept_ref, ritz_ref, *rest):
    if half == 1:
        out, spectrum, expanders, stage, sems, side = rest
        show = pltpu.make_async_copy(ritz_ref, spectrum, side)
        show.start()
    else:
        _, out, expanders, stage, sems = rest
    count = bases_ref.shape[0]
    group = kept_ref.shape[0]
    _, lane = iotas((64, 128))
    for i in range(count):
        basis = bases_ref[i, :64].astype(jnp.float32)
        expanders[i, :64] = jnp.where(lane < 64, basis, -basis).astype(jnp.bfloat16)
        expanders[i, 64:] = pltpu.roll(basis, 64, 1).astype(jnp.bfloat16)

    def copy(i):
        dest = out.at[place_of(i, half, order, group)]
        return pltpu.make_async_copy(stage.at[i], dest, sems.at[i])

    @pl.loop(0, count, step=8)
    def _(i):
        for j in range(8):
            rows = kept_ref[place_of(i + j, half, order, group)]
            stage[i + j] = nn(expanders[i + j], rows).astype(jnp.bfloat16)
            copy(i + j).start()

    @pl.loop(0, count)
    def _(i):
        copy(i).wait()

    if half == 1:
        show.wait()


def compiler(mib):
    return pltpu.CompilerParams(vmem_limit_bytes=mib * 2**20)


def shards(coeffs, weights, mode_counts, owner_order):
    fgroup, _, blocks, points = coeffs.shape
    freqs = lax.axis_size("freq")
    plane = lax.axis_size(PLANE)
    slots = fgroup * freqs
    rows = coeffs.reshape(fgroup, 2 * blocks, points)
    f32, bf16 = jnp.float32, jnp.bfloat16
    packed = jax.ShapeDtypeStruct((plane, 32, 128), f32)
    in_hbm = [
        pltpu.with_memory_space_constraint(x, pltpu.HBM)
        for x in (owner_order, mode_counts, weights)
    ]
    send, own, kept, order, counts = pl.pallas_call(
        gram_kernel,
        out_shape=(
            packed,
            packed,
            pltpu.VMEM((fgroup, 2 * blocks, points), bf16),
            pltpu.SMEM((slots,), jnp.int32),
            pltpu.SMEM((slots,), jnp.int32),
        ),
        in_specs=[HBM_SPEC] * 4,
        out_specs=(VMEM_SPEC, VMEM_SPEC, VMEM_SPEC, SMEM_SPEC, SMEM_SPEC),
        scratch_shapes=[
            pltpu.VMEM((points,), f32),
            pltpu.VMEM((8, points), f32),
            pltpu.VMEM((fgroup, 32, 128), f32),
            pltpu.VMEM((UNROLL, 128, 128), f32),
            pltpu.VMEM((UNROLL, 128, 128), f32),
            pltpu.SemaphoreType.DMA((3,)),
            pltpu.SemaphoreType.DMA((fgroup // UNROLL,)),
        ],
        compiler_params=compiler(32),
        name="gram",
    )(*in_hbm, rows)
    swap = [(0, 1), (1, 0)]
    mine = own + lax.ppermute(send, CORE, swap)
    parts = lax.all_to_all(mine, PLANE, 0, 0, tiled=True)
    payload, ritz = pl.pallas_call(
        solve_kernel,
        out_shape=(pltpu.VMEM((plane, PAY, 128), bf16), pltpu.VMEM((1, M), f32)),
        in_specs=[SMEM_SPEC, SMEM_SPEC, VMEM_SPEC],
        out_specs=(VMEM_SPEC, VMEM_SPEC),
        scratch_shapes=[pltpu.VMEM((BLK, BLK, 128), f32)],
        compiler_params=compiler(16),
        name="solve",
    )(order, counts, parts)
    bases = lax.all_to_all(payload, PLANE, 0, 0, tiled=True)
    others = lax.ppermute(bases, CORE, swap)

    def total(b):
        tail = b[:, 64:66].astype(f32).sum(axis=0)
        return tail[0, :64] + tail[0, 64:] + tail[1, :64]

    def modes(half, bases, *into):
        out = jax.ShapeDtypeStruct((fgroup, 2 * blocks, points), bf16)
        shown = jax.ShapeDtypeStruct((1, M), f32)
        return pl.pallas_call(
            functools.partial(modes_kernel, half),
            out_shape=(out, shown) if half == 1 else out,
            in_specs=[SMEM_SPEC, VMEM_SPEC, VMEM_SPEC, VMEM_SPEC] + [HBM_SPEC] * len(into),
            out_specs=(HBM_SPEC, HBM_SPEC) if half == 1 else HBM_SPEC,
            scratch_shapes=[
                pltpu.VMEM((plane, 128, 128), bf16),
                pltpu.VMEM((plane, 2 * blocks, points), bf16),
                pltpu.SemaphoreType.DMA((plane,)),
            ]
            + [pltpu.SemaphoreType.DMA] * half,
            input_output_aliases={4: 0} if into else {},
            cost_estimate=pl.CostEstimate(
                flops=2 * plane * 128 * 128 * points,
                bytes_accessed=plane * 128 * points * 2,
                transcendentals=0,
            ),
            compiler_params=compiler(16),
            name="modes%d" % half,
        )(order, bases, kept, ritz, *into)

    fields, spectrum = modes(1, bases)
    fields = modes(0, others, fields)
    energy = total(bases) + total(others)
    ring = [
        lax.ppermute(energy, "freq", [(i, (i + k) % freqs) for i in range(freqs)])
        for k in range(1, freqs)
    ]
    energy = functools.reduce(jnp.add, ring, energy) / (fgroup * freqs)
    return (fields.reshape(fgroup, 2, M, points), spectrum, energy)


def solution(mesh):
    split = Mesh(
        mesh.devices.reshape(4, 4, 2, mesh.shape["freq"]), ("space_0", "space_1", "space_2", "freq")
    )
    placed = (P("freq", None, None, SPACE), P(SPACE), P(), P())
    return jax.shard_map(
        shards,
        mesh=split,
        in_specs=placed,
        out_specs=(P("freq", None, None, SPACE), P(SPACE_FREQ, None), P()),
        check_vma=False,
    )
```

```python
import functools

import jax
import jax.numpy as jnp
from jax import lax
from jax.experimental import pallas as pl
from jax.experimental.pallas import tpu as pltpu
from jax.sharding import Mesh
from jax.sharding import PartitionSpec as P

M = 64
ITERS = 3
SPACE = ("space_0", "space_1", "space_2")
PLANE = ("space_0", "space_1")
CORE = "space_2"
SPACE_FREQ = ("space_0", "space_1", "space_2", "freq")
HIGH = lax.Precision.HIGHEST
BLK = 16
PAY = 72
UNROLL = 4
FLIGHT = 4

VMEM_SPEC = pl.BlockSpec(memory_space=pltpu.VMEM)
ANY_SPEC = pl.BlockSpec(memory_space=pl.ANY)
SMEM_SPEC = pl.BlockSpec(memory_space=pltpu.SMEM)
HBM_SPEC = pl.BlockSpec(memory_space=pltpu.HBM)


def nt(a, b, precision=None):
    return lax.dot_general(
        a, b, (((1,), (1,)), ((), ())), precision=precision, preferred_element_type=jnp.float32
    )


def nn(a, b, precision=None):
    return lax.dot_general(
        a, b, (((1,), (0,)), ((), ())), precision=precision, preferred_element_type=jnp.float32
    )


def iotas(shape):
    return (
        lax.broadcasted_iota(jnp.int32, shape, 0),
        lax.broadcasted_iota(jnp.int32, shape, 1),
    )


def here():
    group, core = lax.axis_index("freq"), lax.axis_index(CORE)
    plane = lax.axis_index(PLANE[0]) * lax.axis_size(PLANE[1]) + lax.axis_index(PLANE[1])
    return group, core, plane


def slot_of(plane, core, group):
    return (plane * lax.axis_size(CORE) + core) * lax.axis_size("freq") + group


def place_of(i, half, order, per_group):
    group, core, _ = here()
    return order[slot_of(i, core if half == 1 else 1 - core, group)] - group * per_group


def fold_pack(prod):
    sym = prod + prod.T
    top = sym[:64]
    bot = pltpu.roll(sym[64:], 64, 1)
    _, lane = iotas((64, 128))
    both = 0.5 * jnp.where(lane < 64, top + bot, top - bot)
    row, lane = iotas((32, 128))
    up, low = both[:32], both[32:]
    left = pltpu.roll(low, 96, 1)
    right = pltpu.roll(low, 32, 1)
    out = jnp.where((lane < 32) & (lane < row), left, up)
    inner = (lane >= 64) & (lane < 96)
    out = jnp.where(inner & (lane - 64 < row), left, out)
    return jnp.where(inner & (lane - 64 == row), right, out)


def unpack(packed):
    row, lane = iotas((32, 128))
    turned = jnp.concatenate([packed, jnp.zeros((96, 128), jnp.float32)], axis=0).T
    t0, t1, t2, t3 = (turned[32 * k : 32 * k + 32] for k in range(4))
    t2 = pltpu.roll(t2, 64, 1)
    t3 = pltpu.roll(t3, 64, 1)
    inner = lane - 64
    cr00 = jnp.where(lane >= row, packed, t0)
    ci00 = jnp.where(inner > row, packed, jnp.where(inner == row, 0.0, -t2))
    upper = jnp.where(lane < 32, cr00, jnp.where((lane >= 64) & (lane < 96), ci00, packed))
    diag = pltpu.roll(packed, 64, 1)
    cr11 = jnp.where(lane < row, packed, jnp.where(lane == row, diag, t0))
    ci11 = jnp.where(inner < row, packed, jnp.where(inner == row, 0.0, -t2))
    both11 = pltpu.roll(jnp.where(lane < 64, cr11, ci11), 32, 1)
    ends = jnp.where(lane < 64, t1, -t3)
    second = ((lane >= 32) & (lane < 64)) | (lane >= 96)
    lower = jnp.where(second, both11, ends)
    return jnp.concatenate([upper, lower], axis=0)


def gram_kernel(order_hbm, counts_hbm, cells_hbm, coeffs, *rest):
    send_ref, own_ref, kept_ref, order, counts, cells, wide, packs, even, odd, side, sems = rest
    count = kept_ref.shape[0]
    chunks = count // UNROLL

    def fetch(k):
        part = pl.ds(k * UNROLL, UNROLL)
        return pltpu.make_async_copy(coeffs.at[part], kept_ref.at[part], sems.at[k])

    take_order = pltpu.make_async_copy(order_hbm, order, side.at[0])
    take_cells = pltpu.make_async_copy(cells_hbm, cells, side.at[1])
    take_counts = pltpu.make_async_copy(counts_hbm, counts, side.at[2])
    take_cells.start()
    for k in range(FLIGHT):
        fetch(k).start()
    take_order.start()
    take_counts.start()
    take_cells.wait()
    total = cells.shape[-1] * lax.axis_size(SPACE)
    wide[...] = jnp.broadcast_to(cells[...].reshape(1, -1) / total, wide.shape)

    def product(f):
        rows = kept_ref[f]
        scaled = rows.astype(jnp.float32).reshape(-1, *wide.shape) * wide[...]
        return nt(rows, scaled.reshape(rows.shape).astype(jnp.bfloat16))

    def arrived(k):
        fetch(k).wait()

        @pl.when(k + FLIGHT < chunks)
        def _():
            fetch(k + FLIGHT).start()

    def chunk(k, done, fill):
        for j in range(UNROLL):
            packs[(k - 1) * UNROLL + j] = fold_pack(done[j])
            fill[j] = product(k * UNROLL + j)

    arrived(0)
    for j in range(UNROLL):
        even[j] = product(j)

    @pl.loop(1, chunks - 1, step=2)
    def _(k):
        arrived(k)
        arrived(k + 1)
        chunk(k, even, odd)
        chunk(k + 1, odd, even)

    arrived(chunks - 1)
    chunk(chunks - 1, even, odd)
    for j in range(UNROLL):
        packs[count - UNROLL + j] = fold_pack(odd[j])
    take_order.wait()
    take_counts.wait()
    for half, out_ref in ((0, send_ref), (1, own_ref)):
        for i in range(count // 2):
            out_ref[i] = packs[place_of(i, half, order, count)]


def orth_rows(zt, held):
    n = zt.shape[0]
    gram = nt(zt, zt, HIGH)
    rest_g, rest_z = gram, zt
    row, _ = iotas((BLK, 128))
    outs = []
    for blk in range(n // BLK):
        r0 = BLK * blk
        head_g, head_z = rest_g[:BLK], rest_z[:BLK]
        more = n - r0 - BLK
        tail_g, tail_z = (rest_g[BLK:], rest_z[BLK:]) if more else (None, None)
        for j in range(BLK):
            held[j] = jnp.broadcast_to(head_g[:, r0 + j : r0 + j + 1], (BLK, 128))
        cols = [held[j] for j in range(BLK)]
        tails = [
            jnp.broadcast_to(tail_g[:, r0 + j : r0 + j + 1], (more, 128)) if more else None
            for j in range(BLK)
        ]
        acc = jnp.zeros((BLK, 128), jnp.float32)
        for j in range(BLK):
            here = row == j
            pivot = jnp.broadcast_to(cols[j][j : j + 1], (BLK, 128))
            acc = jnp.where(here, head_z * lax.rsqrt(pivot), acc)
            inv = 1.0 / pivot

            def eliminated(x, j=j, here=here, inv=inv, width=128):
                lead = jnp.broadcast_to(x[j : j + 1], x.shape) * inv[:, :width]
                return jnp.where(here[:, :width], lead, x - cols[j][:, :width] * lead)

            head_z = eliminated(head_z)
            if more:
                head_g = eliminated(head_g, width=n)
            for jj in range(j + 1, BLK):
                cols[jj] = eliminated(cols[jj])
        outs.append(acc)
        for j in range(BLK if more else 0):
            tail_z = tail_z - tails[j] * head_z[j : j + 1]
            tail_g = tail_g - tails[j][:, :n] * head_g[j : j + 1]
        rest_g, rest_z = tail_g, tail_z
    return jnp.concatenate(outs, axis=0)


def solve_kernel(order, counts, parts_ref, pay_ref, ritz_ref, held):
    summed = parts_ref[0]
    for i in range(1, parts_ref.shape[0]):
        summed = summed + parts_ref[i]
    both = unpack(summed)
    row, lane = iotas((64, 128))
    trace = jnp.sum(jnp.where(row == lane, both, 0.0)) * (1.0 / 64.0)
    shift = jnp.full((1, 1), trace)
    hermit = jnp.concatenate([jnp.where(lane < 64, both, -both), pltpu.roll(both, 64, 1)], axis=0)
    row, lane = iotas((128, 128))
    eye = jnp.where(row == lane, 1.0, 0.0)
    shifted = hermit * (1.0 / shift) + eye
    spread = jnp.sum(both * both) * 2.0
    mild = spread <= 512.0 * trace * trace
    start = jnp.where(mild, shifted[:64], eye[:64])
    sweeps = jnp.where(mild, ITERS - 1, ITERS)
    basis = lax.fori_loop(
        0, sweeps, lambda _, rows: orth_rows(nn(rows, shifted, HIGH), held), start
    )
    quad = basis * nn(basis, hermit, HIGH)
    ritz = nt(jnp.ones((8, 128), jnp.float32), quad, HIGH)
    group, core, plane = here()
    kept = counts[order[slot_of(plane, core, group)]]
    _, lane = iotas((8, 64))
    ritz = jnp.where(lane < kept, ritz, 0.0)
    ritz_ref[...] = ritz[:1]
    row, _ = iotas((64, 128))
    sent = jnp.where(row < kept, basis, 0.0).astype(jnp.bfloat16)
    one = ritz.astype(jnp.bfloat16)
    left = ritz - one.astype(jnp.float32)
    two = left.astype(jnp.bfloat16)
    three = left - two.astype(jnp.float32)
    row, _ = iotas((8, 128))
    upper = jnp.concatenate([one.astype(jnp.float32), two.astype(jnp.float32)], axis=1)
    lower = jnp.concatenate([three, jnp.zeros_like(three)], axis=1)
    tail = jnp.where(row == 0, upper, jnp.where(row == 1, lower, 0.0))
    tail = tail.astype(jnp.bfloat16)
    for i in range(pay_ref.shape[0]):
        pay_ref[i, :64] = sent
        pay_ref[i, 64:] = tail


def modes_kernel(half, order, bases_ref, kept_ref, ritz_ref, *rest):
    if half == 1:
        out, spectrum, expanders, stage, sems, side = rest
        show = pltpu.make_async_copy(ritz_ref, spectrum, side)
        show.start()
    else:
        _, out, expanders, stage, sems = rest
    count = bases_ref.shape[0]
    group = kept_ref.shape[0]
    _, lane = iotas((64, 128))
    for i in range(count):
        basis = bases_ref[i, :64].astype(jnp.float32)
        expanders[i, :64] = jnp.where(lane < 64, basis, -basis).astype(jnp.bfloat16)
        expanders[i, 64:] = pltpu.roll(basis, 64, 1).astype(jnp.bfloat16)

    def copy(i):
        dest = out.at[place_of(i, half, order, group)]
        return pltpu.make_async_copy(stage.at[i], dest, sems.at[i])

    @pl.loop(0, count, step=8)
    def _(i):
        for j in range(8):
            rows = kept_ref[place_of(i + j, half, order, group)]
            stage[i + j] = nn(expanders[i + j], rows).astype(jnp.bfloat16)
            copy(i + j).start()

    @pl.loop(0, count)
    def _(i):
        copy(i).wait()

    if half == 1:
        show.wait()


def compiler(mib):
    return pltpu.CompilerParams(vmem_limit_bytes=mib * 2**20)


def shards(coeffs, weights, mode_counts, owner_order):
    fgroup, _, blocks, points = coeffs.shape
    freqs = lax.axis_size("freq")
    plane = lax.axis_size(PLANE)
    slots = fgroup * freqs
    rows = coeffs.reshape(fgroup, 2 * blocks, points)
    f32, bf16 = jnp.float32, jnp.bfloat16
    packed = jax.ShapeDtypeStruct((plane, 32, 128), f32)
    in_hbm = [
        pltpu.with_memory_space_constraint(x, pltpu.HBM)
        for x in (owner_order, mode_counts, weights)
    ]
    send, own, kept, order, counts = pl.pallas_call(
        gram_kernel,
        out_shape=(
            packed,
            packed,
            pltpu.VMEM((fgroup, 2 * blocks, points), bf16),
            pltpu.SMEM((slots,), jnp.int32),
            pltpu.SMEM((slots,), jnp.int32),
        ),
        in_specs=[HBM_SPEC] * 4,
        out_specs=(VMEM_SPEC, VMEM_SPEC, VMEM_SPEC, SMEM_SPEC, SMEM_SPEC),
        scratch_shapes=[
            pltpu.VMEM((points,), f32),
            pltpu.VMEM((8, points), f32),
            pltpu.VMEM((fgroup, 32, 128), f32),
            pltpu.VMEM((UNROLL, 128, 128), f32),
            pltpu.VMEM((UNROLL, 128, 128), f32),
            pltpu.SemaphoreType.DMA((3,)),
            pltpu.SemaphoreType.DMA((fgroup // UNROLL,)),
        ],
        compiler_params=compiler(32),
        name="gram",
    )(*in_hbm, rows)
    swap = [(0, 1), (1, 0)]
    mine = own + lax.ppermute(send, CORE, swap)
    parts = lax.all_to_all(mine, PLANE, 0, 0, tiled=True)
    payload, ritz = pl.pallas_call(
        solve_kernel,
        out_shape=(pltpu.VMEM((plane, PAY, 128), bf16), pltpu.VMEM((1, M), f32)),
        in_specs=[SMEM_SPEC, SMEM_SPEC, VMEM_SPEC],
        out_specs=(VMEM_SPEC, VMEM_SPEC),
        scratch_shapes=[pltpu.VMEM((BLK, BLK, 128), f32)],
        compiler_params=compiler(16),
        name="solve",
    )(order, counts, parts)
    bases = lax.all_to_all(payload, PLANE, 0, 0, tiled=True)
    others = lax.ppermute(bases, CORE, swap)

    def total(b):
        tail = b[:, 64:66].astype(f32).sum(axis=0)
        return tail[0, :64] + tail[0, 64:] + tail[1, :64]

    def modes(half, bases, *into):
        out = jax.ShapeDtypeStruct((fgroup, 2 * blocks, points), bf16)
        shown = jax.ShapeDtypeStruct((1, M), f32)
        return pl.pallas_call(
            functools.partial(modes_kernel, half),
            out_shape=(out, shown) if half == 1 else out,
            in_specs=[SMEM_SPEC, VMEM_SPEC, VMEM_SPEC, VMEM_SPEC] + [HBM_SPEC] * len(into),
            out_specs=(HBM_SPEC, HBM_SPEC) if half == 1 else HBM_SPEC,
            scratch_shapes=[
                pltpu.VMEM((plane, 128, 128), bf16),
                pltpu.VMEM((plane, 2 * blocks, points), bf16),
                pltpu.SemaphoreType.DMA((plane,)),
            ]
            + [pltpu.SemaphoreType.DMA] * half,
            input_output_aliases={4: 0} if into else {},
            cost_estimate=pl.CostEstimate(
                flops=2 * plane * 128 * 128 * points,
                bytes_accessed=plane * 128 * points * 2,
                transcendentals=0,
            ),
            compiler_params=compiler(16),
            name="modes%d" % half,
        )(order, bases, kept, ritz, *into)

    fields, spectrum = modes(1, bases)
    fields = modes(0, others, fields)
    energy = total(bases) + total(others)
    ring = [
        lax.ppermute(energy, "freq", [(i, (i + k) % freqs) for i in range(freqs)])
        for k in range(1, freqs)
    ]
    energy = functools.reduce(jnp.add, ring, energy) / (fgroup * freqs)
    return (fields.reshape(fgroup, 2, M, points), spectrum, energy)


def solution(mesh):
    split = Mesh(
        mesh.devices.reshape(4, 4, 2, mesh.shape["freq"]), ("space_0", "space_1", "space_2", "freq")
    )
    placed = (P("freq", None, None, SPACE), P(SPACE), P(), P())
    return jax.shard_map(
        shards,
        mesh=split,
        in_specs=placed,
        out_specs=(P("freq", None, None, SPACE), P(SPACE_FREQ, None), P()),
        check_vma=False,
    )
```

```python
import functools

import jax
import jax.numpy as jnp
from jax import lax
from jax.experimental import pallas as pl
from jax.experimental.pallas import tpu as pltpu
from jax.sharding import Mesh
from jax.sharding import PartitionSpec as P

M = 64
ITERS = 3
SPACE = ("space_0", "space_1", "space_2")
PLANE = ("space_0", "space_1")
CORE = "space_2"
SPACE_FREQ = ("space_0", "space_1", "space_2", "freq")
HIGH = lax.Precision.HIGHEST
BLK = 16
PAY = 72
UNROLL = 4
FLIGHT = 4

VMEM_SPEC = pl.BlockSpec(memory_space=pltpu.VMEM)
ANY_SPEC = pl.BlockSpec(memory_space=pl.ANY)
SMEM_SPEC = pl.BlockSpec(memory_space=pltpu.SMEM)
HBM_SPEC = pl.BlockSpec(memory_space=pltpu.HBM)


def nt(a, b, precision=None):
    return lax.dot_general(
        a, b, (((1,), (1,)), ((), ())), precision=precision, preferred_element_type=jnp.float32
    )


def nn(a, b, precision=None):
    return lax.dot_general(
        a, b, (((1,), (0,)), ((), ())), precision=precision, preferred_element_type=jnp.float32
    )


def iotas(shape):
    return (
        lax.broadcasted_iota(jnp.int32, shape, 0),
        lax.broadcasted_iota(jnp.int32, shape, 1),
    )


def here():
    group, core = lax.axis_index("freq"), lax.axis_index(CORE)
    plane = lax.axis_index(PLANE[0]) * lax.axis_size(PLANE[1]) + lax.axis_index(PLANE[1])
    return group, core, plane


def slot_of(plane, core, group):
    return (plane * lax.axis_size(CORE) + core) * lax.axis_size("freq") + group


def place_of(i, half, order, per_group):
    group, core, _ = here()
    return order[slot_of(i, core if half == 1 else 1 - core, group)] - group * per_group


def fold_pack(prod):
    sym = prod + prod.T
    top = sym[:64]
    bot = pltpu.roll(sym[64:], 64, 1)
    _, lane = iotas((64, 128))
    both = 0.5 * jnp.where(lane < 64, top + bot, top - bot)
    row, lane = iotas((32, 128))
    up, low = both[:32], both[32:]
    left = pltpu.roll(low, 96, 1)
    right = pltpu.roll(low, 32, 1)
    out = jnp.where((lane < 32) & (lane < row), left, up)
    inner = (lane >= 64) & (lane < 96)
    out = jnp.where(inner & (lane - 64 < row), left, out)
    return jnp.where(inner & (lane - 64 == row), right, out)


def unpack(packed):
    row, lane = iotas((32, 128))
    turned = jnp.concatenate([packed, jnp.zeros((96, 128), jnp.float32)], axis=0).T
    t0, t1, t2, t3 = (turned[32 * k : 32 * k + 32] for k in range(4))
    t2 = pltpu.roll(t2, 64, 1)
    t3 = pltpu.roll(t3, 64, 1)
    inner = lane - 64
    cr00 = jnp.where(lane >= row, packed, t0)
    ci00 = jnp.where(inner > row, packed, jnp.where(inner == row, 0.0, -t2))
    upper = jnp.where(lane < 32, cr00, jnp.where((lane >= 64) & (lane < 96), ci00, packed))
    diag = pltpu.roll(packed, 64, 1)
    cr11 = jnp.where(lane < row, packed, jnp.where(lane == row, diag, t0))
    ci11 = jnp.where(inner < row, packed, jnp.where(inner == row, 0.0, -t2))
    both11 = pltpu.roll(jnp.where(lane < 64, cr11, ci11), 32, 1)
    ends = jnp.where(lane < 64, t1, -t3)
    second = ((lane >= 32) & (lane < 64)) | (lane >= 96)
    lower = jnp.where(second, both11, ends)
    return jnp.concatenate([upper, lower], axis=0)


def gram_kernel(order_hbm, counts_hbm, cells_hbm, coeffs, *rest):
    send_ref, own_ref, kept_ref, order, counts, cells, wide, packs, even, odd, side, sems = rest
    count = kept_ref.shape[0]
    chunks = count // UNROLL

    def fetch(k):
        part = pl.ds(k * UNROLL, UNROLL)
        return pltpu.make_async_copy(coeffs.at[part], kept_ref.at[part], sems.at[k])

    take_order = pltpu.make_async_copy(order_hbm, order, side.at[0])
    take_cells = pltpu.make_async_copy(cells_hbm, cells, side.at[1])
    take_counts = pltpu.make_async_copy(counts_hbm, counts, side.at[2])
    take_cells.start()
    for k in range(FLIGHT):
        fetch(k).start()
    take_order.start()
    take_counts.start()
    take_cells.wait()
    total = cells.shape[-1] * lax.axis_size(SPACE)
    wide[...] = jnp.broadcast_to(cells[...].reshape(1, -1) / total, wide.shape)

    def product(f):
        rows = kept_ref[f]
        scaled = rows.astype(jnp.float32).reshape(-1, *wide.shape) * wide[...]
        return nt(rows, scaled.reshape(rows.shape).astype(jnp.bfloat16))

    def arrived(k):
        fetch(k).wait()

        @pl.when(k + FLIGHT < chunks)
        def _():
            fetch(k + FLIGHT).start()

    def chunk(k, done, fill):
        for j in range(UNROLL):
            packs[(k - 1) * UNROLL + j] = fold_pack(done[j])
            fill[j] = product(k * UNROLL + j)

    arrived(0)
    for j in range(UNROLL):
        even[j] = product(j)

    @pl.loop(1, chunks - 1, step=2)
    def _(k):
        arrived(k)
        arrived(k + 1)
        chunk(k, even, odd)
        chunk(k + 1, odd, even)

    arrived(chunks - 1)
    chunk(chunks - 1, even, odd)
    for j in range(UNROLL):
        packs[count - UNROLL + j] = fold_pack(odd[j])
    take_order.wait()
    take_counts.wait()
    for half, out_ref in ((0, send_ref), (1, own_ref)):
        for i in range(count // 2):
            out_ref[i] = packs[place_of(i, half, order, count)]


def orth_rows(zt, held):
    n = zt.shape[0]
    gram = nt(zt, zt, HIGH)
    rest_g, rest_z = gram, zt
    row, _ = iotas((BLK, 128))
    outs = []
    for blk in range(n // BLK):
        r0 = BLK * blk
        head_g, head_z = rest_g[:BLK], rest_z[:BLK]
        more = n - r0 - BLK
        tail_g, tail_z = (rest_g[BLK:], rest_z[BLK:]) if more else (None, None)
        for j in range(BLK):
            held[j] = jnp.broadcast_to(head_g[:, r0 + j : r0 + j + 1], (BLK, 128))
        cols = [held[j] for j in range(BLK)]
        tails = [
            jnp.broadcast_to(tail_g[:, r0 + j : r0 + j + 1], (more, 128)) if more else None
            for j in range(BLK)
        ]
        acc = jnp.zeros((BLK, 128), jnp.float32)
        for j in range(BLK):
            here = row == j
            pivot = jnp.broadcast_to(cols[j][j : j + 1], (BLK, 128))
            acc = jnp.where(here, head_z * lax.rsqrt(pivot), acc)
            inv = 1.0 / pivot

            def eliminated(x, j=j, here=here, inv=inv, width=128):
                lead = jnp.broadcast_to(x[j : j + 1], x.shape) * inv[:, :width]
                return jnp.where(here[:, :width], lead, x - cols[j][:, :width] * lead)

            head_z = eliminated(head_z)
            if more:
                head_g = eliminated(head_g, width=n)
            for jj in range(j + 1, BLK):
                cols[jj] = eliminated(cols[jj])
        outs.append(acc)
        for j in range(BLK if more else 0):
            tail_z = tail_z - tails[j] * head_z[j : j + 1]
            tail_g = tail_g - tails[j][:, :n] * head_g[j : j + 1]
        rest_g, rest_z = tail_g, tail_z
    return jnp.concatenate(outs, axis=0)


def solve_kernel(order, counts, parts_ref, pay_ref, ritz_ref, held):
    summed = parts_ref[0]
    for i in range(1, parts_ref.shape[0]):
        summed = summed + parts_ref[i]
    both = unpack(summed)
    row, lane = iotas((64, 128))
    trace = jnp.sum(jnp.where(row == lane, both, 0.0)) * (1.0 / 64.0)
    shift = jnp.full((1, 1), trace)
    hermit = jnp.concatenate([jnp.where(lane < 64, both, -both), pltpu.roll(both, 64, 1)], axis=0)
    row, lane = iotas((128, 128))
    eye = jnp.where(row == lane, 1.0, 0.0)
    shifted = hermit * (1.0 / shift) + eye
    spread = jnp.sum(both * both) * 2.0
    mild = spread <= 512.0 * trace * trace
    start = jnp.where(mild, shifted[:64], eye[:64])
    sweeps = jnp.where(mild, ITERS - 1, ITERS)
    basis = lax.fori_loop(
        0, sweeps, lambda _, rows: orth_rows(nn(rows, shifted, HIGH), held), start
    )
    quad = basis * nn(basis, hermit, HIGH)
    ritz = nt(jnp.ones((8, 128), jnp.float32), quad, HIGH)
    group, core, plane = here()
    kept = counts[order[slot_of(plane, core, group)]]
    _, lane = iotas((8, 64))
    ritz = jnp.where(lane < kept, ritz, 0.0)
    ritz_ref[...] = ritz[:1]
    row, _ = iotas((64, 128))
    sent = jnp.where(row < kept, basis, 0.0).astype(jnp.bfloat16)
    one = ritz.astype(jnp.bfloat16)
    left = ritz - one.astype(jnp.float32)
    two = left.astype(jnp.bfloat16)
    three = left - two.astype(jnp.float32)
    row, _ = iotas((8, 128))
    upper = jnp.concatenate([one.astype(jnp.float32), two.astype(jnp.float32)], axis=1)
    lower = jnp.concatenate([three, jnp.zeros_like(three)], axis=1)
    tail = jnp.where(row == 0, upper, jnp.where(row == 1, lower, 0.0))
    tail = tail.astype(jnp.bfloat16)
    for i in range(pay_ref.shape[0]):
        pay_ref[i, :64] = sent
        pay_ref[i, 64:] = tail


def modes_kernel(half, order, bases_ref, kept_ref, ritz_ref, *rest):
    if half == 1:
        out, spectrum, expanders, stage, sems, side = rest
        show = pltpu.make_async_copy(ritz_ref, spectrum, side)
        show.start()
    else:
        _, out, expanders, stage, sems = rest
    count = bases_ref.shape[0]
    group = kept_ref.shape[0]
    _, lane = iotas((64, 128))
    for i in range(count):
        basis = bases_ref[i, :64].astype(jnp.float32)
        expanders[i, :64] = jnp.where(lane < 64, basis, -basis).astype(jnp.bfloat16)
        expanders[i, 64:] = pltpu.roll(basis, 64, 1).astype(jnp.bfloat16)

    def copy(i):
        dest = out.at[place_of(i, half, order, group)]
        return pltpu.make_async_copy(stage.at[i], dest, sems.at[i])

    @pl.loop(0, count, step=8)
    def _(i):
        for j in range(8):
            rows = kept_ref[place_of(i + j, half, order, group)]
            stage[i + j] = nn(expanders[i + j], rows).astype(jnp.bfloat16)
            copy(i + j).start()

    @pl.loop(0, count)
    def _(i):
        copy(i).wait()

    if half == 1:
        show.wait()


def compiler(mib):
    return pltpu.CompilerParams(vmem_limit_bytes=mib * 2**20)


def shards(coeffs, weights, mode_counts, owner_order):
    fgroup, _, blocks, points = coeffs.shape
    freqs = lax.axis_size("freq")
    plane = lax.axis_size(PLANE)
    slots = fgroup * freqs
    rows = coeffs.reshape(fgroup, 2 * blocks, points)
    f32, bf16 = jnp.float32, jnp.bfloat16
    packed = jax.ShapeDtypeStruct((plane, 32, 128), f32)
    in_hbm = [
        pltpu.with_memory_space_constraint(x, pltpu.HBM)
        for x in (owner_order, mode_counts, weights)
    ]
    send, own, kept, order, counts = pl.pallas_call(
        gram_kernel,
        out_shape=(
            packed,
            packed,
            pltpu.VMEM((fgroup, 2 * blocks, points), bf16),
            pltpu.SMEM((slots,), jnp.int32),
            pltpu.SMEM((slots,), jnp.int32),
        ),
        in_specs=[HBM_SPEC] * 4,
        out_specs=(VMEM_SPEC, VMEM_SPEC, VMEM_SPEC, SMEM_SPEC, SMEM_SPEC),
        scratch_shapes=[
            pltpu.VMEM((points,), f32),
            pltpu.VMEM((8, points), f32),
            pltpu.VMEM((fgroup, 32, 128), f32),
            pltpu.VMEM((UNROLL, 128, 128), f32),
            pltpu.VMEM((UNROLL, 128, 128), f32),
            pltpu.SemaphoreType.DMA((3,)),
            pltpu.SemaphoreType.DMA((fgroup // UNROLL,)),
        ],
        compiler_params=compiler(32),
        name="gram",
    )(*in_hbm, rows)
    swap = [(0, 1), (1, 0)]
    mine = own + lax.ppermute(send, CORE, swap)
    parts = lax.all_to_all(mine, PLANE, 0, 0, tiled=True)
    payload, ritz = pl.pallas_call(
        solve_kernel,
        out_shape=(pltpu.VMEM((plane, PAY, 128), bf16), pltpu.VMEM((1, M), f32)),
        in_specs=[SMEM_SPEC, SMEM_SPEC, VMEM_SPEC],
        out_specs=(VMEM_SPEC, VMEM_SPEC),
        scratch_shapes=[pltpu.VMEM((BLK, BLK, 128), f32)],
        compiler_params=compiler(16),
        name="solve",
    )(order, counts, parts)
    bases = lax.all_to_all(payload, PLANE, 0, 0, tiled=True)
    others = lax.ppermute(bases, CORE, swap)

    def total(b):
        tail = b[:, 64:66].astype(f32).sum(axis=0)
        return tail[0, :64] + tail[0, 64:] + tail[1, :64]

    def modes(half, bases, *into):
        out = jax.ShapeDtypeStruct((fgroup, 2 * blocks, points), bf16)
        shown = jax.ShapeDtypeStruct((1, M), f32)
        return pl.pallas_call(
            functools.partial(modes_kernel, half),
            out_shape=(out, shown) if half == 1 else out,
            in_specs=[SMEM_SPEC, VMEM_SPEC, VMEM_SPEC, VMEM_SPEC] + [HBM_SPEC] * len(into),
            out_specs=(HBM_SPEC, HBM_SPEC) if half == 1 else HBM_SPEC,
            scratch_shapes=[
                pltpu.VMEM((plane, 128, 128), bf16),
                pltpu.VMEM((plane, 2 * blocks, points), bf16),
                pltpu.SemaphoreType.DMA((plane,)),
            ]
            + [pltpu.SemaphoreType.DMA] * half,
            input_output_aliases={4: 0} if into else {},
            cost_estimate=pl.CostEstimate(
                flops=2 * plane * 128 * 128 * points,
                bytes_accessed=plane * 128 * points * 2,
                transcendentals=0,
            ),
            compiler_params=compiler(16),
            name="modes%d" % half,
        )(order, bases, kept, ritz, *into)

    fields, spectrum = modes(1, bases)
    fields = modes(0, others, fields)
    energy = total(bases) + total(others)
    one, two, three = (
        lax.ppermute(energy, "freq", [(i, i ^ k) for i in range(freqs)]) for k in (1, 2, 3)
    )
    energy = ((energy + one) + (two + three)) / (fgroup * freqs)
    return (fields.reshape(fgroup, 2, M, points), spectrum, energy)


def solution(mesh):
    split = Mesh(
        mesh.devices.reshape(4, 4, 2, mesh.shape["freq"]), ("space_0", "space_1", "space_2", "freq")
    )
    placed = (P("freq", None, None, SPACE), P(SPACE), P(), P())
    return jax.shard_map(
        shards,
        mesh=split,
        in_specs=placed,
        out_specs=(P("freq", None, None, SPACE), P(SPACE_FREQ, None), P()),
        check_vma=False,
    )
```
